8 devices in a mesh: dp: 1 (over z), tp: 8 (over x, y, core).
Axes of the slice: x: 2, y: 2, z: 1, core: 2. Of those that a mesh axis runs over, the one named last changes fastest.
Arguments:
- x: bfloat16 [1024, 8192], P(('dp', 'tp'))
- gain_a: bfloat16 [8192], replicated
- wq: bfloat16 [8192, 8192], P(None, 'tp')
- wk: bfloat16 [8192, 8192], P(None, 'tp')
- wv: bfloat16 [8192, 8192], P(None, 'tp')
- wo: bfloat16 [8192, 8192], P('tp')
- gain_m: bfloat16 [8192], replicated
- w_gate: bfloat16 [8192, 24576], P(None, 'tp')
- w_up: bfloat16 [8192, 24576], P(None, 'tp')
- w_down: bfloat16 [24576, 8192], P('tp')
Outputs:
- output: bfloat16 [1024, 8192], P(('dp', 'tp'))
All inputs are finite; a program needn't handle non-finite values.
Results may differ from the reference program's by a relative error of at most 0.017.
Values are sent between devices in bfloat16 or wider.
A program may use at most 2 GiB of HBM per device.

```python
import jax
import jax.numpy as jnp
from jax import lax

ROWS = 1024
D = 8192
HEADS = 64
KV_HEADS = 64
HEAD = 128
FF = 24576
THETA = 10000


def setup_inputs(seed: int = 0, part: int = 0) -> dict:
    kx, kn, kq, kk, kv, ko, km, kg, ku, kd = jax.random.split(jax.random.key(seed), 10)

    def weights(key, rows, columns):
        return jax.random.normal(key, (rows, columns), jnp.float32) * rows**-0.5

    drawn = {
        "x": jax.random.normal(jax.random.fold_in(kx, part), (ROWS, D), jnp.float32),
        "gain_a": 1 + 0.1 * jax.random.normal(kn, (D,), jnp.float32),
        "wq": 2 * weights(kq, D, HEADS * HEAD),
        "wk": 2 * weights(kk, D, KV_HEADS * HEAD),
        "wv": 4 * weights(kv, D, KV_HEADS * HEAD),
        "wo": weights(ko, HEADS * HEAD, D),
        "gain_m": 1 + 0.1 * jax.random.normal(km, (D,), jnp.float32),
        "w_gate": weights(kg, D, FF),
        "w_up": weights(ku, D, FF),
        "w_down": 2 * weights(kd, FF, D),
    }
    return {k: v.astype(jnp.bfloat16) for k, v in drawn.items()}


def normed(x, gain):
    wide = x.astype(jnp.float32)
    scale = lax.rsqrt(jnp.mean(wide * wide, -1, keepdims=True) + 1e-6)
    return (wide * scale * gain.astype(jnp.float32)).astype(jnp.bfloat16)


def turned(t, place, theta):
    half = t.shape[-1] // 2
    angle = place.astype(jnp.float32)[:, None] * theta ** (-jnp.arange(half, dtype=jnp.float32) / half)
    cos, sin = jnp.cos(angle)[:, None], jnp.sin(angle)[:, None]
    a, b = t[..., :half].astype(jnp.float32), t[..., half:].astype(jnp.float32)
    return jnp.concatenate([a * cos - b * sin, b * cos + a * sin], -1).astype(jnp.bfloat16)


def matmul(a, w):
    return jnp.dot(a, w, preferred_element_type=jnp.float32).astype(jnp.bfloat16)


def einsum(form, a, b):
    return jnp.einsum(form, a.astype(jnp.float32), b.astype(jnp.float32))


def attention(q, k, v):
    scores = einsum("tgsd,ugd->gstu", q, k) * q.shape[-1] ** -0.5
    token = jnp.arange(q.shape[0])
    scores = jnp.where(token[:, None] >= token, scores, -jnp.inf)
    weights = jax.nn.softmax(scores, -1).astype(jnp.bfloat16)
    return einsum("gstu,ugd->tgsd", weights, v).astype(jnp.bfloat16)


def reference(x, gain_a, wq, wk, wv, wo, gain_m, w_gate, w_up, w_down):
    a, place = normed(x, gain_a), jnp.arange(ROWS)
    q = turned(matmul(a, wq).reshape(ROWS, HEADS, HEAD), place, THETA).reshape(ROWS, KV_HEADS, -1, HEAD)
    k = turned(matmul(a, wk).reshape(ROWS, KV_HEADS, HEAD), place, THETA)
    v = matmul(a, wv).reshape(ROWS, KV_HEADS, HEAD)
    seen = attention(q, k, v).reshape(ROWS, HEADS * HEAD)
    h = (x.astype(jnp.float32) + jnp.dot(seen, wo, preferred_element_type=jnp.float32)).astype(jnp.bfloat16)
    b = normed(h, gain_m)
    gate = jnp.dot(b, w_gate, preferred_element_type=jnp.float32)
    up = jnp.dot(b, w_up, preferred_element_type=jnp.float32)
    hidden = (jax.nn.silu(gate) * up).astype(jnp.bfloat16)
    return (h.astype(jnp.float32) + jnp.dot(hidden, w_down, preferred_element_type=jnp.float32)).astype(jnp.bfloat16)
```

```python
import functools

import jax
import jax.numpy as jnp
from jax import lax
from jax.experimental import pallas as pl
from jax.experimental.pallas import tpu as pltpu
from jax.sharding import PartitionSpec as P

HEAD = 128
THETA = 10000
N = 8
HALF = 64
ORDER = (1, 3, 5, 7, 0, 2, 4, 6)
LOG2E = 1.4426950408889634
HIDDEN = -2e30
X, Y, C = ([(i, i ^ bit) for i in range(N)] for bit in (4, 2, 1))


def pp(t, pairs):
    return lax.ppermute(t, "tp", pairs)


def normed(x, gain):
    wide = x.astype(jnp.float32)
    scale = lax.rsqrt(jnp.mean(wide * wide, -1, keepdims=True) + 1e-6)
    return (wide * scale * gain.astype(jnp.float32)).astype(jnp.bfloat16)


def tables(rows):
    half = HEAD // 2
    angle = jnp.arange(rows).astype(jnp.float32)[:, None] * THETA ** (-jnp.arange(half, dtype=jnp.float32) / half)
    cos, sin = jnp.cos(angle), jnp.sin(angle)
    return jnp.concatenate([cos, cos], -1), jnp.concatenate([-sin, sin], -1)


def turn(t, cos, sin):
    wide = t.astype(jnp.float32)
    swapped = jnp.concatenate([wide[:, HEAD // 2 :], wide[:, : HEAD // 2]], axis=1)
    return (wide * cos + swapped * sin).astype(jnp.bfloat16)


def _dot(a, b, ca, cb):
    return lax.dot_general(a, b, (((ca,), (cb,)), ((), ())), preferred_element_type=jnp.float32)


def _attend(me_ref, q_ref, ka_ref, kb_ref, va_ref, vb_ref, cos_ref, sin_ref, o_ref, q_s, k_s, v_s, *, which):
    me = me_ref[0]
    places = []
    for j in range(N):
        o = jnp.bitwise_xor(me, j)
        at = pl.ds(pl.multiple_of(((1 - (o & 1)) * 4 + lax.shift_right_logical(o, 1)) * HALF, HALF), HALF)
        places.append(at)
        for half, (k_ref, v_ref) in enumerate(((ka_ref, va_ref), (kb_ref, vb_ref))):
            to = slice(j * 2 * HALF + half * HALF, j * 2 * HALF + (half + 1) * HALF)
            k_s[to, :] = turn(k_ref[at, :], cos_ref[to, :], sin_ref[to, :])
            v_s[to, :] = v_ref[at, :]
        of = slice(j * 2 * HALF + which * HALF, j * 2 * HALF + (which + 1) * HALF)
        q_s[j * HALF : (j + 1) * HALF, :] = turn(q_ref[at, :], cos_ref[of, :], sin_ref[of, :])
    tile = 2 * HALF
    for u in range(N // 2):
        keys = 4 * HALF * (u + 1)
        s = _dot(q_s[u * tile : (u + 1) * tile, :], k_s[:keys, :], 1, 1)
        row = lax.broadcasted_iota(jnp.int32, (tile, 4 * HALF), 0)
        token = row + jnp.where(row >= HALF, HALF, 0) + which * HALF
        ok = lax.broadcasted_iota(jnp.int32, (tile, 4 * HALF), 1) <= token
        last = jnp.where(ok, s[:, keys - 4 * HALF :], HIDDEN)
        s = last if u == 0 else jnp.concatenate([s[:, : keys - 4 * HALF], last], axis=1)
        p = jnp.exp2((s - s.max(axis=1, keepdims=True)) * (HEAD**-0.5 * LOG2E))
        total = p.sum(axis=1, keepdims=True)
        out = (_dot(p.astype(jnp.bfloat16), v_s[:keys, :], 1, 0) * (1 / total)).astype(jnp.bfloat16)
        for i in range(2):
            o_ref[places[2 * u + i], :] = out[i * HALF : (i + 1) * HALF, :]


def attend(me, q, ks, vs, cos, sin, which):
    rows, width = q.shape
    part = pl.BlockSpec((rows, HEAD), lambda h, _: (0, h))
    whole = pl.BlockSpec(cos.shape, lambda h, _: (0, 0))
    keys = 2 * rows
    return pl.pallas_call(
        functools.partial(_attend, which=which),
        grid_spec=pltpu.PrefetchScalarGridSpec(
            num_scalar_prefetch=1,
            grid=(width // HEAD,),
            in_specs=[part] * 5 + [whole] * 2,
            out_specs=part,
            scratch_shapes=[pltpu.VMEM((rows, HEAD), jnp.bfloat16), pltpu.VMEM((keys, HEAD), jnp.bfloat16), pltpu.VMEM((keys, HEAD), jnp.bfloat16)],
        ),
        out_shape=jax.ShapeDtypeStruct(q.shape, q.dtype),
        compiler_params=pltpu.CompilerParams(dimension_semantics=("arbitrary",), vmem_limit_bytes=48 * 2**20),
        cost_estimate=pl.CostEstimate(flops=4 * rows * keys * width, transcendentals=rows * keys * width // HEAD, bytes_accessed=12 * rows * width),
        name=f"attend{which}",
    )(me, q, *ks, *vs, cos, sin)


def gathered(p):
    cut = p.shape[0] // 2
    c = pp(p, C)
    x, y = pp(p, X), pp(p, Y)
    d = jnp.concatenate([pp(x[:cut], Y), pp(y[cut:], X)])
    return jnp.concatenate([c, pp(y, C), pp(x, C), pp(d, C), p, y, x, d])


def scattered(res, t, w):
    rows = t.shape[0] // 2
    n = rows // 4
    cut = n // 2
    away = jnp.dot(t[:rows], w, preferred_element_type=jnp.float32).astype(jnp.bfloat16)
    got = pp(away, C)
    mine = jnp.dot(t[rows:], w, preferred_element_type=jnp.float32) + got.astype(jnp.float32)
    own, y, x, d = (mine[i * n : (i + 1) * n] for i in range(4))
    d = d.astype(jnp.bfloat16)
    low, high = pp(d[:cut], X), pp(d[cut:], Y)
    y0 = pp((y[:cut] + low.astype(jnp.float32)).astype(jnp.bfloat16), Y)
    x1 = pp((x[cut:] + high.astype(jnp.float32)).astype(jnp.bfloat16), X)
    y1 = pp(y[cut:].astype(jnp.bfloat16), Y)
    x0 = pp(x[:cut].astype(jnp.bfloat16), X)
    own = own + jnp.concatenate([x0, x1]).astype(jnp.float32) + jnp.concatenate([y0, y1]).astype(jnp.float32)
    return (res.astype(jnp.float32) + own).astype(jnp.bfloat16)


def matmul(a, w):
    return jnp.dot(a, w, preferred_element_type=jnp.float32).astype(jnp.bfloat16)


def solution(mesh):
    def step(x, gain_a, wq, wk, wv, wo, gain_m, w_gate, w_up, w_down):
        me = lax.axis_index("tp").astype(jnp.int32)[None]
        cos, sin = tables(N * x.shape[0])
        halves = (slice(0, HALF), slice(HALF, 2 * HALF))
        a = normed(x, gain_a)
        some = [gathered(a[h]) for h in halves]
        qs, ks, vs = ([matmul(s, w) for s in some] for w in (wq, wk, wv))
        out = []
        for which, h in enumerate(halves):
            seen = attend(me, qs[which], ks, vs, cos, sin, which)
            h = scattered(x[h], seen, wo)
            b = gathered(normed(h, gain_m))
            gate = jnp.dot(b, w_gate, preferred_element_type=jnp.float32)
            up = jnp.dot(b, w_up, preferred_element_type=jnp.float32)
            hidden = (jax.nn.silu(gate) * up).astype(jnp.bfloat16)
            out.append(scattered(h, hidden, w_down))
        return jnp.concatenate(out)

    tokens, columns, rows_of = P(("dp", "tp"), None), P(None, "tp"), P("tp", None)
    return jax.shard_map(
        step,
        mesh=mesh,
        in_specs=(tokens, P(None), columns, columns, columns, rows_of, P(None), columns, columns, rows_of),
        out_specs=tokens,
        check_vma=False,
    )
```

```python
import functools

import jax
import jax.numpy as jnp
from jax import lax
from jax.experimental import pallas as pl
from jax.experimental.pallas import tpu as pltpu
from jax.sharding import PartitionSpec as P

HEAD = 128
THETA = 10000
N = 8
OWN = 128
X, Y, C = 4, 2, 1
PLACE = {0: 0, 1: 1, 4: 2, 5: 3, 2: 4, 3: 5, 6: 6, 7: 7}
LOG2E = 1.4426950408889634
HIDDEN = -2e30
BIG = 63 * 2**20
MESH = pl.DeviceIdType.MESH
ANY = pl.BlockSpec(memory_space=pl.ANY)
INSIDE = pl.BlockSpec(memory_space=pltpu.VMEM)


def _dot(a, b, ca, cb):
    return lax.dot_general(a, b, (((ca,), (cb,)), ((), ())), preferred_element_type=jnp.float32)


def _peer(bit):
    return {"tp": jnp.bitwise_xor(lax.axis_index("tp"), bit)}


def _meet():
    barrier = pltpu.get_barrier_semaphore()
    for bit in (X, Y, C):
        pl.semaphore_signal(barrier, inc=1, device_id=_peer(bit), device_id_type=MESH)
    pl.semaphore_wait(barrier, 3)


def tables(rows):
    half = HEAD // 2
    angle = jnp.arange(rows).astype(jnp.float32)[:, None] * THETA ** (-jnp.arange(half, dtype=jnp.float32) / half)
    cos, sin = jnp.cos(angle), jnp.sin(angle)
    return jnp.concatenate([cos, cos], -1), jnp.concatenate([-sin, sin], -1)


def turn(t, cos, sin):
    wide = t.astype(jnp.float32)
    swapped = jnp.concatenate([wide[:, HEAD // 2 :], wide[:, : HEAD // 2]], axis=1)
    return (wide * cos + swapped * sin).astype(jnp.bfloat16)


def _attend(me_ref, q_ref, k_ref, v_ref, cos_ref, sin_ref, o_ref, q_s, k_s, v_s):
    me = me_ref[0]
    places = []
    for j in range(N):
        o = jnp.bitwise_xor(me, j)
        place = (o & 1) + (o & 2) * 2 + lax.shift_right_logical(o & 4, 1)
        at = pl.ds(pl.multiple_of(place * OWN, OWN), OWN)
        places.append(at)
        to = slice(j * OWN, (j + 1) * OWN)
        cos, sin = cos_ref[to, :], sin_ref[to, :]
        k_s[to, :] = turn(k_ref[at, :], cos, sin)
        q_s[to, :] = turn(q_ref[at, :], cos, sin)
        v_s[to, :] = v_ref[at, :]
    tile = 2 * OWN
    ok = lax.broadcasted_iota(jnp.int32, (tile, tile), 0) <= lax.broadcasted_iota(jnp.int32, (tile, tile), 1)
    for u in range(N // 2):
        keys = tile * (u + 1)
        s = _dot(k_s[:keys, :], q_s[u * tile : keys, :], 1, 1)
        last = jnp.where(ok, s[keys - tile :, :], HIDDEN)
        s = last if u == 0 else jnp.concatenate([s[: keys - tile, :], last], axis=0)
        p = jnp.exp2((s - s.max(axis=0, keepdims=True)) * (HEAD**-0.5 * LOG2E))
        total = p.sum(axis=0, keepdims=True)
        out = (_dot(v_s[:keys, :], p.astype(jnp.bfloat16), 0, 0) * (1 / total)).T.astype(jnp.bfloat16)
        for i in range(2):
            o_ref[places[2 * u + i], :] = out[i * OWN : (i + 1) * OWN, :]


def attend(q, k, v, cos, sin):
    rows, width = q.shape
    part = pl.BlockSpec((rows, HEAD), lambda h, _: (0, h))
    whole = pl.BlockSpec(cos.shape, lambda h, _: (0, 0))
    return pl.pallas_call(
        _attend,
        grid_spec=pltpu.PrefetchScalarGridSpec(
            num_scalar_prefetch=1,
            grid=(width // HEAD,),
            in_specs=[part] * 3 + [whole] * 2,
            out_specs=part,
            scratch_shapes=[pltpu.VMEM((rows, HEAD), jnp.bfloat16)] * 3,
        ),
        out_shape=jax.ShapeDtypeStruct(q.shape, q.dtype),
        compiler_params=pltpu.CompilerParams(dimension_semantics=("arbitrary",), vmem_limit_bytes=48 * 2**20),
        cost_estimate=pl.CostEstimate(flops=4 * rows * rows * width, transcendentals=rows * rows * width // HEAD, bytes_accessed=8 * rows * width),
        name="attend",
    )(lax.axis_index("tp").astype(jnp.int32)[None], q, k, v, cos, sin)


KC = 1024
WIDE = 512
SLOTS = 4
KINDS = {
    "c": (PLACE[0] * OWN, OWN, PLACE[1] * OWN, C),
    "x": (PLACE[0] * OWN, OWN, PLACE[4] * OWN, X),
    "y": (PLACE[0] * OWN, OWN, PLACE[2] * OWN, Y),
    "xc": (PLACE[4] * OWN, OWN, PLACE[5] * OWN, C),
    "yc": (PLACE[2] * OWN, OWN, PLACE[3] * OWN, C),
    "dt": (PLACE[4] * OWN, OWN // 2, PLACE[6] * OWN, Y),
    "db": (PLACE[2] * OWN + OWN // 2, OWN // 2, PLACE[6] * OWN + OWN // 2, X),
    "dc": (PLACE[6] * OWN, OWN, PLACE[7] * OWN, C),
}


def _gather_matmul(*refs, n, epilogue, cut_last):
    x_ref, gain_ref = refs[:2]
    w_refs = refs[2 : 2 + n]
    outs = refs[2 + n : -6]
    all_s, acc_s, ring, w_sem, s_sem, r_sem = refs[-6:]
    chunks, steps = all_s.shape[0], acc_s.shape[0]
    d = chunks * KC
    rows = N * OWN
    uses = (chunks + 2 + (1 if cut_last else 0)) * steps

    def load(u):
        c = jnp.clip(lax.div(u, steps) - 2, 0, chunks - 1)
        s = lax.rem(u, steps)
        return [
            pltpu.make_async_copy(
                w.at[pl.ds(pl.multiple_of(c * KC, KC), KC), pl.ds(pl.multiple_of(s * WIDE, WIDE), WIDE)],
                ring.at[lax.rem(u, SLOTS), :, pl.ds(i * WIDE, WIDE)],
                w_sem.at[lax.rem(u, SLOTS), i],
            )
            for i, w in enumerate(w_refs)
        ]

    def copy(kind, c):
        at, size, to, bit = KINDS[kind]
        i = list(KINDS).index(kind)
        return pltpu.make_async_remote_copy(
            src_ref=all_s.at[c, pl.ds(at, size)], dst_ref=all_s.at[c, pl.ds(to, size)], send_sem=s_sem.at[i, c], recv_sem=r_sem.at[i, c],
            device_id=_peer(bit), device_id_type=MESH)

    def start(c, *kinds):
        for kind in kinds:
            copy(kind, c).start()

    def wait(c, *kinds):
        for kind in kinds:
            copy(kind, c).wait_recv()

    def when(flag, then):
        if isinstance(flag, bool):
            if flag:
                then()
        else:
            pl.when(flag)(then)

    def forward(c):
        wait(c, "x", "y")
        start(c, "dt", "db", "xc", "yc")
        when(c + 2 < chunks, lambda: start(c + 2, "x", "y", "c"))

    def finish(c):
        wait(c, "dt", "db")
        start(c, "dc")

    for u in range(SLOTS - 1):
        for part in load(u):
            part.start()

    def norm(i, _):
        some = pl.ds(pl.multiple_of(i * 16, 16), 16)
        total = jnp.zeros((16, 1), jnp.float32)
        for c in range(chunks):
            wide = x_ref[some, c * KC : (c + 1) * KC].astype(jnp.float32)
            total += jnp.sum(wide * wide, axis=1, keepdims=True)
        scale = lax.rsqrt(total * (1 / d) + 1e-6)
        for c in range(chunks):
            wide = x_ref[some, c * KC : (c + 1) * KC].astype(jnp.float32)
            all_s[c, some, :] = (wide * scale * gain_ref[:, c * KC : (c + 1) * KC].astype(jnp.float32)).astype(jnp.bfloat16)

    lax.fori_loop(0, OWN // 16, norm, None)
    _meet()
    start(0, "x", "y", "c")

    def block(u, c, at, size, mode):
        s, slot = lax.rem(u, steps), lax.rem(u, SLOTS)

        @pl.when(u + SLOTS - 1 < uses)
        def _():
            for part in load(u + SLOTS - 1):
                part.start()

        for part in load(u):
            part.wait()
        got = _dot(all_s[c, at : at + size, :], ring[slot], 1, 0)
        if mode != "first":
            got += acc_s[s, at : at + size, :]
        if mode != "last":
            acc_s[s, at : at + size, :] = got
        else:
            epilogue([got[:, i * WIDE : (i + 1) * WIDE] for i in range(n)], outs, slice(at, at + size), pl.ds(pl.multiple_of(s * WIDE, WIDE), WIDE))

    def run(first, c, at, size, mode, early=None):
        def body(s, _):
            if early is not None:
                pl.when(s == 0)(lambda: forward(early))
                pl.when(s == steps - 1)(lambda: finish(early))
            block(first + s, c, at, size, mode)

        lax.fori_loop(0, steps, body, None)

    wait(0, "c")
    run(0, 0, 0, 2 * OWN, "first")
    wait(0, "x", "y")
    start(0, "dt", "db", "xc", "yc")
    start(1, "x", "y", "c")
    start(2, "x", "y", "c")
    wait(0, "xc", "yc")
    run(steps, 0, 2 * OWN, 4 * OWN, "first")
    finish(0)
    wait(0, "dc")
    run(2 * steps, 0, 6 * OWN, 2 * OWN, "first", 1)

    def middle(c, _):
        wait(c, "c", "xc", "yc", "dc")
        run((c + 2) * steps, c, 0, rows, "middle", c + 1)

    if cut_last:
        c = chunks - 1
        lax.fori_loop(1, c - 1, middle, None)
        wait(c - 1, "c", "xc", "yc", "dc")

        def body(s, _):
            pl.when(s == 0)(lambda: forward(c))
            block((c + 1) * steps + s, c - 1, 0, rows, "middle")

        lax.fori_loop(0, steps, body, None)
        wait(c, "c", "xc", "yc")
        run((c + 2) * steps, c, 0, 6 * OWN, "last")
        finish(c)
        wait(c, "dc")
        run((c + 3) * steps, c, 6 * OWN, 2 * OWN, "last")
    else:
        lax.fori_loop(1, chunks - 1, middle, None)
        wait(chunks - 1, "c", "xc", "yc", "dc")
        run((chunks + 1) * steps, chunks - 1, 0, rows, "last")

    def drain(c, _):
        for kind in KINDS:
            copy(kind, c).wait_send()

    lax.fori_loop(0, chunks, drain, None)


def gather_matmul(x, gain, weights, outs, epilogue, collective_id, cut_last, name):
    own, d = x.shape
    rows, width, n = N * own, weights[0].shape[1], len(weights)
    chunks, steps = d // KC, width // WIDE
    return pl.pallas_call(
        functools.partial(_gather_matmul, n=n, epilogue=epilogue, cut_last=cut_last),
        in_specs=[INSIDE, INSIDE] + [ANY] * n,
        out_specs=[INSIDE] * outs,
        out_shape=[jax.ShapeDtypeStruct((rows, width), jnp.bfloat16)] * outs,
        scratch_shapes=[
            pltpu.VMEM((chunks, rows, KC), jnp.bfloat16),
            pltpu.VMEM((steps, rows, n * WIDE), jnp.float32),
            pltpu.VMEM((SLOTS, KC, n * WIDE), jnp.bfloat16),
            pltpu.SemaphoreType.DMA((SLOTS, n)),
            pltpu.SemaphoreType.DMA((len(KINDS), chunks)),
            pltpu.SemaphoreType.DMA((len(KINDS), chunks)),
        ],
        compiler_params=pltpu.CompilerParams(collective_id=collective_id, has_side_effects=True, vmem_limit_bytes=BIG),
        cost_estimate=pl.CostEstimate(flops=2 * rows * d * width * n, transcendentals=0, bytes_accessed=2 * d * width * n),
        name=name,
    )(x, gain[None], *weights)


def rounded(parts, outs, rows, columns):
    for part, out in zip(parts, outs):
        out[rows, columns] = part.astype(jnp.bfloat16)


def gated(parts, outs, rows, columns):
    gate, up = parts
    outs[0][rows, columns] = (gate * (1 / (1 + jnp.exp(-gate))) * up).astype(jnp.bfloat16)


NC = 256
KEEP = 8
HALF = OWN // 2


def _matmul_scatter(t_ref, res_ref, w_ref, out_ref, ring, away, mine, d_s, x_s, y_s, c_r, low_r, high_r, x_r, y_r, w_sem, s_sem, r_sem):
    chunks = c_r.shape[0]
    top, bottom = pl.ds(0, HALF), pl.ds(HALF, HALF)

    def load(i):
        return pltpu.make_async_copy(w_ref.at[:, pl.ds(pl.multiple_of(i * NC, NC), NC)], ring.at[lax.rem(i, SLOTS)], w_sem.at[lax.rem(i, SLOTS)])

    def copy(kind, i):
        k = lax.rem(i, KEEP)
        src, dst, bit = {
            "c": (away.at[k], c_r.at[i], C),
            "low": (d_s.at[k, top], low_r.at[i], X),
            "high": (d_s.at[k, bottom], high_r.at[i], Y),
            "x0": (x_s.at[k, top], x_r.at[i, top], X),
            "x1": (x_s.at[k, bottom], x_r.at[i, bottom], X),
            "y0": (y_s.at[k, top], y_r.at[i, top], Y),
            "y1": (y_s.at[k, bottom], y_r.at[i, bottom], Y),
        }[kind]
        j = ("c", "low", "high", "x0", "x1", "y0", "y1").index(kind)
        return pltpu.make_async_remote_copy(src_ref=src, dst_ref=dst, send_sem=s_sem.at[j, i], recv_sem=r_sem.at[j, i], device_id=_peer(bit),
                                            device_id_type=MESH)

    for i in range(SLOTS - 1):
        load(i).start()
    _meet()

    def multiply(i):
        k = lax.rem(i, KEEP)

        @pl.when(i + SLOTS - 1 < chunks)
        def _():
            load(i + SLOTS - 1).start()

        load(i).wait()
        got = _dot(t_ref[...], ring[lax.rem(i, SLOTS)], 1, 0)
        for b in range(4):
            away[k, b * OWN : (b + 1) * OWN, :] = got[(2 * b + 1) * OWN : (2 * b + 2) * OWN, :].astype(jnp.bfloat16)
            mine[k, b * OWN : (b + 1) * OWN, :] = got[2 * b * OWN : (2 * b + 1) * OWN, :]
        copy("c", i).start()

    def pair(i):
        k = lax.rem(i, KEEP)
        copy("c", i).wait_recv()
        sums = [mine[k, b * OWN : (b + 1) * OWN, :] + c_r[i, b * OWN : (b + 1) * OWN, :].astype(jnp.float32) for b in range(4)]
        d_s[k] = sums[3].astype(jnp.bfloat16)
        x_s[k, :HALF, :] = sums[1][:HALF].astype(jnp.bfloat16)
        y_s[k, HALF:, :] = sums[2][HALF:].astype(jnp.bfloat16)
        for kind in ("low", "high", "x0", "y1"):
            copy(kind, i).start()
        for b in range(3):
            mine[k, b * OWN : (b + 1) * OWN, :] = sums[b]
        copy("c", i).wait_send()

    def pass_on(i):
        k = lax.rem(i, KEEP)
        copy("low", i).wait_recv()
        y_s[k, :HALF, :] = (mine[k, 2 * OWN : 2 * OWN + HALF, :] + low_r[i].astype(jnp.float32)).astype(jnp.bfloat16)
        copy("y0", i).start()
        copy("high", i).wait_recv()
        x_s[k, HALF:, :] = (mine[k, OWN + HALF : 2 * OWN, :] + high_r[i].astype(jnp.float32)).astype(jnp.bfloat16)
        copy("x1", i).start()

    def finish(i):
        k = lax.rem(i, KEEP)
        for kind in ("x0", "x1", "y0", "y1"):
            copy(kind, i).wait_recv()
        columns = pl.ds(pl.multiple_of(i * NC, NC), NC)
        total = mine[k, :OWN, :] + x_r[i].astype(jnp.float32) + y_r[i].astype(jnp.float32)
        out_ref[:, columns] = (res_ref[:, columns].astype(jnp.float32) + total).astype(jnp.bfloat16)
        for kind in ("low", "high", "x0", "x1", "y0", "y1"):
            copy(kind, i).wait_send()

    def step(i, _):
        pl.when((i >= 6) & (i < chunks + 6))(lambda: finish(i - 6))
        pl.when((i >= 4) & (i < chunks + 4))(lambda: pass_on(i - 4))
        pl.when((i >= 2) & (i < chunks + 2))(lambda: pair(i - 2))
        pl.when(i < chunks)(lambda: multiply(i))

    lax.fori_loop(0, chunks + 6, step, None)


def matmul_scatter(res, t, w, collective_id, name):
    rows, depth = t.shape
    d = w.shape[1]
    chunks = d // NC
    sent = lambda *shape: pltpu.VMEM((*shape, NC), jnp.bfloat16)
    return pl.pallas_call(
        _matmul_scatter,
        in_specs=[INSIDE, INSIDE, ANY],
        out_specs=INSIDE,
        out_shape=jax.ShapeDtypeStruct(res.shape, res.dtype),
        scratch_shapes=[
            pltpu.VMEM((SLOTS, depth, NC), jnp.bfloat16),
            sent(KEEP, rows // 2),
            pltpu.VMEM((KEEP, rows // 2, NC), jnp.float32),
            sent(KEEP, OWN), sent(KEEP, OWN), sent(KEEP, OWN),
            sent(chunks, rows // 2), sent(chunks, HALF), sent(chunks, HALF), sent(chunks, OWN), sent(chunks, OWN),
            pltpu.SemaphoreType.DMA((SLOTS,)),
            pltpu.SemaphoreType.DMA((7, chunks)),
            pltpu.SemaphoreType.DMA((7, chunks)),
        ],
        compiler_params=pltpu.CompilerParams(collective_id=collective_id, has_side_effects=True, vmem_limit_bytes=BIG),
        cost_estimate=pl.CostEstimate(flops=2 * rows * depth * d, transcendentals=0, bytes_accessed=2 * depth * d),
        name=name,
    )(t, res, w)


def solution(mesh):
    def step(x, gain_a, wq, wk, wv, wo, gain_m, w_gate, w_up, w_down):
        cos, sin = tables(N * x.shape[0])
        q, k, v = gather_matmul(x, gain_a, (wq, wk, wv), 3, rounded, 0, True, "qkv")
        seen = attend(q, k, v, cos, sin)
        h = matmul_scatter(x, seen, wo, 1, "wo")
        (hidden,) = gather_matmul(h, gain_m, (w_gate, w_up), 1, gated, 2, False, "gate_up")
        return matmul_scatter(h, hidden, w_down, 3, "down")

    tokens, columns, rows_of = P(("dp", "tp"), None), P(None, "tp"), P("tp", None)
    return jax.shard_map(
        step,
        mesh=mesh,
        in_specs=(tokens, P(None), columns, columns, columns, rows_of, P(None), columns, columns, rows_of),
        out_specs=tokens,
        check_vma=False,
    )
```

```python
import functools

import jax
import jax.numpy as jnp
from jax import lax
from jax.experimental import pallas as pl
from jax.experimental.pallas import tpu as pltpu
from jax.sharding import PartitionSpec as P

HEAD = 128
THETA = 10000
N = 8
OWN = 128
X, Y, C = 4, 2, 1
PLACE = {0: 0, 1: 1, 4: 2, 5: 3, 2: 4, 3: 5, 6: 6, 7: 7}
LOG2E = 1.4426950408889634
HIDDEN = -2e30
BIG = 63 * 2**20
MESH = pl.DeviceIdType.MESH
ANY = pl.BlockSpec(memory_space=pl.ANY)
INSIDE = pl.BlockSpec(memory_space=pltpu.VMEM)


def _dot(a, b, ca, cb):
    return lax.dot_general(a, b, (((ca,), (cb,)), ((), ())), preferred_element_type=jnp.float32)


def _peer(bit):
    return {"tp": jnp.bitwise_xor(lax.axis_index("tp"), bit)}


def _meet():
    barrier = pltpu.get_barrier_semaphore()
    for bit in (X, Y, C):
        pl.semaphore_signal(barrier, inc=1, device_id=_peer(bit), device_id_type=MESH)
    pl.semaphore_wait(barrier, 3)


def tables(rows):
    half = HEAD // 2
    angle = jnp.arange(rows).astype(jnp.float32)[:, None] * THETA ** (-jnp.arange(half, dtype=jnp.float32) / half)
    return jnp.cos(angle), jnp.sin(angle)


def turn(t, cos, sin):
    wide = t.astype(jnp.float32)
    return (wide * cos + pltpu.roll(wide, HEAD // 2, 1) * sin).astype(jnp.bfloat16)


def _attend(me_ref, q_ref, k_ref, v_ref, cos_ref, sin_ref, o_ref, q_s, k_s, v_s, cos_s, sin_s):
    me = me_ref[0]
    heads = q_ref.shape[1] // HEAD

    @pl.when(pl.program_id(0) == 0)
    def _():
        cos_s[...] = jnp.concatenate([cos_ref[...], cos_ref[...]], axis=1)
        sin_s[...] = jnp.concatenate([-sin_ref[...], sin_ref[...]], axis=1)

    places = []
    for j in range(N):
        o = jnp.bitwise_xor(me, j)
        place = (o & 1) + (o & 2) * 2 + lax.shift_right_logical(o & 4, 1)
        at = pl.ds(pl.multiple_of(place * OWN, OWN), OWN)
        places.append(at)
        to = slice(j * OWN, (j + 1) * OWN)
        cos, sin = cos_s[to, :], sin_s[to, :]
        for h in range(heads):
            columns = slice(h * HEAD, (h + 1) * HEAD)
            k_s[h, to, :] = turn(k_ref[at, columns], cos, sin)
            q_s[h, to, :] = turn(q_ref[at, columns], cos, sin)
            v_s[h, to, :] = v_ref[at, columns]
    tile = 2 * OWN
    ok = lax.broadcasted_iota(jnp.int32, (tile, tile), 0) <= lax.broadcasted_iota(jnp.int32, (tile, tile), 1)
    units = [(u, h) for u in range(N // 2) for h in range(heads)]

    def scores(u, h):
        keys = tile * (u + 1)
        return _dot(k_s[h, :keys, :], q_s[h, u * tile : keys, :], 1, 1)

    def weights(u, s):
        keys = tile * (u + 1)
        last = jnp.where(ok, s[keys - tile :, :], HIDDEN)
        s = last if u == 0 else jnp.concatenate([s[: keys - tile, :], last], axis=0)
        p = jnp.exp2((s - s.max(axis=0, keepdims=True)) * (HEAD**-0.5 * LOG2E))
        return p.astype(jnp.bfloat16), p.sum(axis=0, keepdims=True)

    def results(u, h, p, total):
        keys = tile * (u + 1)
        out = (_dot(v_s[h, :keys, :], p, 0, 0) * (1 / total)).T.astype(jnp.bfloat16)
        for i in range(2):
            o_ref[places[2 * u + i], h * HEAD : (h + 1) * HEAD] = out[i * OWN : (i + 1) * OWN, :]

    ahead = scores(*units[0])
    for i, (u, h) in enumerate(units):
        now = ahead
        if i + 1 < len(units):
            ahead = scores(*units[i + 1])
        results(u, h, *weights(u, now))


HEADS_A_STEP = 2


def attend(q, k, v, cos, sin):
    rows, width = q.shape
    heads = HEADS_A_STEP
    part = pl.BlockSpec((rows, heads * HEAD), lambda h, _: (0, h))
    whole = pl.BlockSpec(cos.shape, lambda h, _: (0, 0))
    return pl.pallas_call(
        _attend,
        grid_spec=pltpu.PrefetchScalarGridSpec(
            num_scalar_prefetch=1,
            grid=(width // HEAD // heads,),
            in_specs=[part] * 3 + [whole] * 2,
            out_specs=part,
            scratch_shapes=[pltpu.VMEM((heads, rows, HEAD), jnp.bfloat16)] * 3 + [pltpu.VMEM((rows, HEAD), jnp.float32)] * 2,
        ),
        out_shape=jax.ShapeDtypeStruct(q.shape, q.dtype),
        compiler_params=pltpu.CompilerParams(dimension_semantics=("arbitrary",), vmem_limit_bytes=BIG),
        cost_estimate=pl.CostEstimate(flops=4 * rows * rows * width, transcendentals=rows * rows * width // HEAD, bytes_accessed=8 * rows * width),
        name="attend",
    )(lax.axis_index("tp").astype(jnp.int32)[None], q, k, v, cos, sin)


KC = 1024
WIDE = 512
SLOTS = 4
LANES = 128
FORWARDS = (0.5, 0.88)
KINDS = {
    "c": (PLACE[0] * OWN, OWN, PLACE[1] * OWN, C),
    "x": (PLACE[0] * OWN, OWN, PLACE[4] * OWN, X),
    "y": (PLACE[0] * OWN, OWN, PLACE[2] * OWN, Y),
    "xc": (PLACE[4] * OWN, OWN, PLACE[5] * OWN, C),
    "yc": (PLACE[2] * OWN, OWN, PLACE[3] * OWN, C),
    "dt": (PLACE[4] * OWN, OWN // 2, PLACE[6] * OWN, Y),
    "db": (PLACE[2] * OWN + OWN // 2, OWN // 2, PLACE[6] * OWN + OWN // 2, X),
    "dc": (PLACE[6] * OWN, OWN, PLACE[7] * OWN, C),
}


def _gather_matmul(*refs, n, epilogue, early):
    x_ref, gain_ref = refs[:2]
    w_refs = refs[2 : 2 + n]
    outs = refs[2 + n : -6]
    all_s, acc_s, ring, w_sem, s_sem, r_sem = refs[-6:]
    chunks, steps = all_s.shape[0], acc_s.shape[0]
    d = chunks * KC
    rows = N * OWN
    cut = early == chunks
    uses = (early + chunks + cut) * steps

    def load(u):
        c = lax.div(u, steps)
        c = jnp.minimum(c - jnp.where(c < early, 0, early), chunks - 1)
        s = lax.rem(u, steps)
        return [
            pltpu.make_async_copy(
                w.at[pl.ds(pl.multiple_of(c * KC, KC), KC), pl.ds(pl.multiple_of(s * WIDE, WIDE), WIDE)],
                ring.at[lax.rem(u, SLOTS), :, pl.ds(i * WIDE, WIDE)],
                w_sem.at[lax.rem(u, SLOTS), i],
            )
            for i, w in enumerate(w_refs)
        ]

    def copy(kind, c):
        at, size, to, bit = KINDS[kind]
        i = list(KINDS).index(kind)
        return pltpu.make_async_remote_copy(
            src_ref=all_s.at[c, pl.ds(at, size)], dst_ref=all_s.at[c, pl.ds(to, size)], send_sem=s_sem.at[i, c], recv_sem=r_sem.at[i, c],
            device_id=_peer(bit), device_id_type=MESH)

    def start(c, *kinds):
        for kind in kinds:
            copy(kind, c).start()

    def wait(c, *kinds):
        for kind in kinds:
            copy(kind, c).wait_recv()

    def when(flag, then):
        if isinstance(flag, bool):
            if flag:
                then()
        else:
            pl.when(flag)(then)

    def forward(c):
        wait(c, "x", "y")
        start(c, "dt", "db", "xc", "yc")
        when(c + 2 < chunks, lambda: start(c + 2, "x", "y"))

    def finish(c):
        wait(c, "dt", "db")
        start(c, "dc")

    for u in range(SLOTS - 1):
        for part in load(u):
            part.start()

    def norm(i, _):
        some = pl.ds(pl.multiple_of(i * 16, 16), 16)
        squares = jnp.zeros((16, LANES), jnp.float32)
        for j in range(d // LANES):
            wide = x_ref[some, j * LANES : (j + 1) * LANES].astype(jnp.float32)
            squares += wide * wide
        scale = lax.rsqrt(jnp.sum(squares, axis=1, keepdims=True) * (1 / d) + 1e-6)
        for j in range(d // LANES):
            wide = x_ref[some, j * LANES : (j + 1) * LANES].astype(jnp.float32)
            at = j * LANES % KC
            all_s[j * LANES // KC, some, at : at + LANES] = (wide * scale * gain_ref[j : j + 1, :].astype(jnp.float32)).astype(jnp.bfloat16)

    lax.fori_loop(0, OWN // 16, norm, None)
    _meet()
    start(0, "x", "y")
    start(1, "x", "y")
    lax.fori_loop(0, chunks, lambda c, _: start(c, "c"), None)

    def block(u, c, at, size, mode):
        s, slot = lax.rem(u, steps), lax.rem(u, SLOTS)

        @pl.when(u + SLOTS - 1 < uses)
        def _():
            for part in load(u + SLOTS - 1):
                part.start()

        for part in load(u):
            part.wait()
        got = _dot(all_s[c, at : at + size, :], ring[slot], 1, 0)
        if mode != "first":
            got += acc_s[s, at : at + size, :]
        if mode != "last":
            acc_s[s, at : at + size, :] = got
        else:
            epilogue([got[:, i * WIDE : (i + 1) * WIDE] for i in range(n)], outs, slice(at, at + size), pl.ds(pl.multiple_of(s * WIDE, WIDE), WIDE))

    def run(first, c, at, size, mode, before=None):
        def body(s, _):
            if before is not None:
                before(s)
            block(first + s, c, at, size, mode)

        lax.fori_loop(0, steps, body, None)

    def first_rows(c, mode):
        wait(c, "c")

        def before(s):
            for k, share in enumerate(FORWARDS):
                pl.when(c * steps + s == int(early * steps * share))(lambda k=k: forward(k))

        run(c * steps, c, 0, 2 * OWN, mode, before)

    first_rows(0, "first")
    lax.fori_loop(1, chunks - 1 if cut else early, lambda c, _: first_rows(c, "middle"), None)
    if cut:
        first_rows(chunks - 1, "last")
    finish(0)

    def chunk(c, at, mode):
        wait(c, *(("xc", "yc", "dc") if at else ("c", "xc", "yc", "dc")))

        def before(s):
            pl.when((s == 0) & (c + 2 < chunks))(lambda: forward(c + 2))
            if not cut:
                pl.when((s == steps - 1) & (c + 1 < chunks))(lambda: finish(c + 1))

        run((early + c) * steps, c, at, rows - at, mode, before)
        if cut:
            pl.when(c + 2 < chunks)(lambda: finish(c + 1))

    chunk(0, 2 * OWN, "first")
    lax.fori_loop(1, chunks - 1 if cut else early, lambda c, _: chunk(c, 2 * OWN, "middle"), None)
    c = chunks - 1
    if cut:
        wait(c, "xc", "yc")
        run((early + c) * steps, c, 2 * OWN, 4 * OWN, "last")
        finish(c)
        wait(c, "dc")
        run((early + c + 1) * steps, c, 6 * OWN, 2 * OWN, "last")
    else:
        lax.fori_loop(early, c, lambda c, _: chunk(c, 0, "middle"), None)
        chunk(c, 0, "last")

    def drain(c, _):
        for kind in KINDS:
            copy(kind, c).wait_send()

    lax.fori_loop(0, chunks, drain, None)


def gather_matmul(x, gain, weights, outs, epilogue, collective_id, early, name):
    own, d = x.shape
    rows, width, n = N * own, weights[0].shape[1], len(weights)
    chunks, steps = d // KC, width // WIDE
    return pl.pallas_call(
        functools.partial(_gather_matmul, n=n, epilogue=epilogue, early=early),
        in_specs=[INSIDE, INSIDE] + [ANY] * n,
        out_specs=[INSIDE] * outs,
        out_shape=[jax.ShapeDtypeStruct((rows, width), jnp.bfloat16)] * outs,
        scratch_shapes=[
            pltpu.VMEM((chunks, rows, KC), jnp.bfloat16),
            pltpu.VMEM((steps, rows, n * WIDE), jnp.float32),
            pltpu.VMEM((SLOTS, KC, n * WIDE), jnp.bfloat16),
            pltpu.SemaphoreType.DMA((SLOTS, n)),
            pltpu.SemaphoreType.DMA((len(KINDS), chunks)),
            pltpu.SemaphoreType.DMA((len(KINDS), chunks)),
        ],
        compiler_params=pltpu.CompilerParams(collective_id=collective_id, has_side_effects=True, vmem_limit_bytes=BIG),
        cost_estimate=pl.CostEstimate(flops=2 * rows * d * width * n, transcendentals=0, bytes_accessed=2 * d * width * n),
        name=name,
    )(x, gain.reshape(-1, LANES), *weights)


def rounded(parts, outs, rows, columns):
    for part, out in zip(parts, outs):
        out[rows, columns] = part.astype(jnp.bfloat16)


def gated(parts, outs, rows, columns):
    gate, up = parts
    outs[0][rows, columns] = (gate * (1 / (1 + jnp.exp(-gate))) * up).astype(jnp.bfloat16)


NC = 256
LAGS = (6, 4, 2)
MULTIPLY_FIRST = False
KEEP = 8
HALF = OWN // 2


def _matmul_scatter(t_ref, res_ref, w_ref, out_ref, ring, away, mine, d_s, x_s, y_s, c_r, low_r, high_r, x_r, y_r, w_sem, s_sem, r_sem):
    chunks = c_r.shape[0]
    top, bottom = pl.ds(0, HALF), pl.ds(HALF, HALF)

    def load(i):
        return pltpu.make_async_copy(w_ref.at[:, pl.ds(pl.multiple_of(i * NC, NC), NC)], ring.at[lax.rem(i, SLOTS)], w_sem.at[lax.rem(i, SLOTS)])

    def copy(kind, i):
        k = lax.rem(i, KEEP)
        src, dst, bit = {
            "c": (away.at[k], c_r.at[i], C),
            "low": (d_s.at[k, top], low_r.at[i], X),
            "high": (d_s.at[k, bottom], high_r.at[i], Y),
            "x0": (x_s.at[k, top], x_r.at[i, top], X),
            "x1": (x_s.at[k, bottom], x_r.at[i, bottom], X),
            "y0": (y_s.at[k, top], y_r.at[i, top], Y),
            "y1": (y_s.at[k, bottom], y_r.at[i, bottom], Y),
        }[kind]
        j = ("c", "low", "high", "x0", "x1", "y0", "y1").index(kind)
        return pltpu.make_async_remote_copy(src_ref=src, dst_ref=dst, send_sem=s_sem.at[j, i], recv_sem=r_sem.at[j, i], device_id=_peer(bit),
                                            device_id_type=MESH)

    for i in range(SLOTS - 1):
        load(i).start()
    _meet()

    def multiply(i):
        k = lax.rem(i, KEEP)

        @pl.when(i + SLOTS - 1 < chunks)
        def _():
            load(i + SLOTS - 1).start()

        load(i).wait()
        got = _dot(t_ref[...], ring[lax.rem(i, SLOTS)], 1, 0)
        for b in range(4):
            away[k, b * OWN : (b + 1) * OWN, :] = got[(2 * b + 1) * OWN : (2 * b + 2) * OWN, :].astype(jnp.bfloat16)
            mine[k, b * OWN : (b + 1) * OWN, :] = got[2 * b * OWN : (2 * b + 1) * OWN, :]
        copy("c", i).start()

    def pair(i):
        k = lax.rem(i, KEEP)
        copy("c", i).wait_recv()
        sums = [mine[k, b * OWN : (b + 1) * OWN, :] + c_r[i, b * OWN : (b + 1) * OWN, :].astype(jnp.float32) for b in range(4)]
        d_s[k] = sums[3].astype(jnp.bfloat16)
        x_s[k, :HALF, :] = sums[1][:HALF].astype(jnp.bfloat16)
        y_s[k, HALF:, :] = sums[2][HALF:].astype(jnp.bfloat16)
        for kind in ("low", "high", "x0", "y1"):
            copy(kind, i).start()
        for b in range(3):
            mine[k, b * OWN : (b + 1) * OWN, :] = sums[b]
        copy("c", i).wait_send()

    def pass_on(i):
        k = lax.rem(i, KEEP)
        copy("low", i).wait_recv()
        y_s[k, :HALF, :] = (mine[k, 2 * OWN : 2 * OWN + HALF, :] + low_r[i].astype(jnp.float32)).astype(jnp.bfloat16)
        copy("y0", i).start()
        copy("high", i).wait_recv()
        x_s[k, HALF:, :] = (mine[k, OWN + HALF : 2 * OWN, :] + high_r[i].astype(jnp.float32)).astype(jnp.bfloat16)
        copy("x1", i).start()

    def finish(i):
        k = lax.rem(i, KEEP)
        for kind in ("x0", "x1", "y0", "y1"):
            copy(kind, i).wait_recv()
        columns = pl.ds(pl.multiple_of(i * NC, NC), NC)
        total = mine[k, :OWN, :] + x_r[i].astype(jnp.float32) + y_r[i].astype(jnp.float32)
        out_ref[:, columns] = (res_ref[:, columns].astype(jnp.float32) + total).astype(jnp.bfloat16)
        for kind in ("low", "high", "x0", "x1", "y0", "y1"):
            copy(kind, i).wait_send()

    def step(i, _):
        if MULTIPLY_FIRST:
            pl.when(i < chunks)(lambda: multiply(i))
        for lag, stage in zip(LAGS, (finish, pass_on, pair)):
            pl.when((i >= lag) & (i < chunks + lag))(lambda lag=lag, stage=stage: stage(i - lag))
        if not MULTIPLY_FIRST:
            pl.when(i < chunks)(lambda: multiply(i))

    lax.fori_loop(0, chunks + LAGS[0], step, None)


def matmul_scatter(res, t, w, collective_id, name):
    rows, depth = t.shape
    d = w.shape[1]
    chunks = d // NC
    sent = lambda *shape: pltpu.VMEM((*shape, NC), jnp.bfloat16)
    return pl.pallas_call(
        _matmul_scatter,
        in_specs=[INSIDE, INSIDE, ANY],
        out_specs=INSIDE,
        out_shape=jax.ShapeDtypeStruct(res.shape, res.dtype),
        scratch_shapes=[
            pltpu.VMEM((SLOTS, depth, NC), jnp.bfloat16),
            sent(KEEP, rows // 2),
            pltpu.VMEM((KEEP, rows // 2, NC), jnp.float32),
            sent(KEEP, OWN), sent(KEEP, OWN), sent(KEEP, OWN),
            sent(chunks, rows // 2), sent(chunks, HALF), sent(chunks, HALF), sent(chunks, OWN), sent(chunks, OWN),
            pltpu.SemaphoreType.DMA((SLOTS,)),
            pltpu.SemaphoreType.DMA((7, chunks)),
            pltpu.SemaphoreType.DMA((7, chunks)),
        ],
        compiler_params=pltpu.CompilerParams(collective_id=collective_id, has_side_effects=True, vmem_limit_bytes=BIG),
        cost_estimate=pl.CostEstimate(flops=2 * rows * depth * d, transcendentals=0, bytes_accessed=2 * depth * d),
        name=name,
    )(t, res, w)


def solution(mesh):
    def step(x, gain_a, wq, wk, wv, wo, gain_m, w_gate, w_up, w_down):
        cos, sin = tables(N * x.shape[0])
        q, k, v = gather_matmul(x, gain_a, (wq, wk, wv), 3, rounded, 0, 8, "qkv")
        seen = attend(q, k, v, cos, sin)
        h = matmul_scatter(x, seen, wo, 1, "wo")
        (hidden,) = gather_matmul(h, gain_m, (w_gate, w_up), 1, gated, 2, 4, "gate_up")
        return matmul_scatter(h, hidden, w_down, 3, "down")

    tokens, columns, rows_of = P(("dp", "tp"), None), P(None, "tp"), P("tp", None)
    return jax.shard_map(
        step,
        mesh=mesh,
        in_specs=(tokens, P(None), columns, columns, columns, rows_of, P(None), columns, columns, rows_of),
        out_specs=tokens,
        check_vma=False,
    )
```

```python
import functools

import jax
import jax.numpy as jnp
import numpy as np
from jax import lax
from jax.experimental import pallas as pl
from jax.experimental.pallas import tpu as pltpu
from jax.sharding import PartitionSpec as P

HEAD = 128
THETA = 10000
N = 8
OWN = 128
X, Y, C = 4, 2, 1
PLACE = {0: 0, 1: 1, 4: 2, 5: 3, 2: 4, 3: 5, 6: 6, 7: 7}
LOG2E = 1.4426950408889634
HIDDEN = -2e30
BIG = 63 * 2**20
MESH = pl.DeviceIdType.MESH
ANY = pl.BlockSpec(memory_space=pl.ANY)
INSIDE = pl.BlockSpec(memory_space=pltpu.VMEM)


def _dot(a, b, ca, cb):
    return lax.dot_general(a, b, (((ca,), (cb,)), ((), ())), preferred_element_type=jnp.float32)


def _peer(bit):
    return {"tp": jnp.bitwise_xor(lax.axis_index("tp"), bit)}


def _meet():
    barrier = pltpu.get_barrier_semaphore()
    for bit in (X, Y, C):
        pl.semaphore_signal(barrier, inc=1, device_id=_peer(bit), device_id_type=MESH)
    pl.semaphore_wait(barrier, 3)


def tables(rows):
    half = HEAD // 2
    angle = np.arange(rows, dtype=np.float32)[:, None] * np.float32(THETA) ** (-np.arange(half, dtype=np.float32) / np.float32(half))
    return jnp.asarray(np.cos(angle)), jnp.asarray(np.sin(angle))


def turn(t, cos, sin):
    wide = t.astype(jnp.float32)
    return (wide * cos + pltpu.roll(wide, HEAD // 2, 1) * sin).astype(jnp.bfloat16)


def _attend(me_ref, q_ref, k_ref, v_ref, cos_ref, sin_ref, o_ref, q_s, k_s, v_s, cos_s, sin_s):
    me = me_ref[0]
    heads = q_ref.shape[1] // HEAD

    @pl.when(pl.program_id(0) == 0)
    def _():
        cos_s[...] = jnp.concatenate([cos_ref[...], cos_ref[...]], axis=1)
        sin_s[...] = jnp.concatenate([-sin_ref[...], sin_ref[...]], axis=1)

    places = []
    for j in range(N):
        o = jnp.bitwise_xor(me, j)
        place = (o & 1) + (o & 2) * 2 + lax.shift_right_logical(o & 4, 1)
        at = pl.ds(pl.multiple_of(place * OWN, OWN), OWN)
        places.append(at)
        to = slice(j * OWN, (j + 1) * OWN)
        cos, sin = cos_s[to, :], sin_s[to, :]
        for h in range(heads):
            columns = slice(h * HEAD, (h + 1) * HEAD)
            k_s[h, to, :] = turn(k_ref[at, columns], cos, sin)
            q_s[h, to, :] = turn(q_ref[at, columns], cos, sin)
            v_s[h, to, :] = v_ref[at, columns]
    tile = 2 * OWN
    ok = lax.broadcasted_iota(jnp.int32, (tile, tile), 0) <= lax.broadcasted_iota(jnp.int32, (tile, tile), 1)
    units = [(u, h) for u in range(N // 2) for h in range(heads)]

    def scores(u, h):
        keys = tile * (u + 1)
        return _dot(k_s[h, :keys, :], q_s[h, u * tile : keys, :], 1, 1)

    def weights(u, s):
        keys = tile * (u + 1)
        last = jnp.where(ok, s[keys - tile :, :], HIDDEN)
        s = last if u == 0 else jnp.concatenate([s[: keys - tile, :], last], axis=0)
        p = jnp.exp2((s - s.max(axis=0, keepdims=True)) * (HEAD**-0.5 * LOG2E))
        return p.astype(jnp.bfloat16), p.sum(axis=0, keepdims=True)

    def results(u, h, p, total):
        keys = tile * (u + 1)
        out = (_dot(v_s[h, :keys, :], p, 0, 0) * (1 / total)).T.astype(jnp.bfloat16)
        for i in range(2):
            o_ref[places[2 * u + i], h * HEAD : (h + 1) * HEAD] = out[i * OWN : (i + 1) * OWN, :]

    ahead = scores(*units[0])
    for i, (u, h) in enumerate(units):
        now = ahead
        if i + 1 < len(units):
            ahead = scores(*units[i + 1])
        results(u, h, *weights(u, now))


HEADS_A_STEP = 2


def attend(q, k, v, cos, sin):
    rows, width = q.shape
    heads = HEADS_A_STEP
    part = pl.BlockSpec((rows, heads * HEAD), lambda h, _: (0, h))
    whole = pl.BlockSpec(cos.shape, lambda h, _: (0, 0))
    return pl.pallas_call(
        _attend,
        grid_spec=pltpu.PrefetchScalarGridSpec(
            num_scalar_prefetch=1,
            grid=(width // HEAD // heads,),
            in_specs=[part] * 3 + [whole] * 2,
            out_specs=part,
            scratch_shapes=[pltpu.VMEM((heads, rows, HEAD), jnp.bfloat16)] * 3 + [pltpu.VMEM((rows, HEAD), jnp.float32)] * 2,
        ),
        out_shape=jax.ShapeDtypeStruct(q.shape, q.dtype),
        compiler_params=pltpu.CompilerParams(dimension_semantics=("arbitrary",), vmem_limit_bytes=BIG),
        cost_estimate=pl.CostEstimate(flops=4 * rows * rows * width, transcendentals=rows * rows * width // HEAD, bytes_accessed=8 * rows * width),
        name="attend",
    )(lax.axis_index("tp").astype(jnp.int32)[None], q, k, v, cos, sin)


KC = 1024
WIDE = 512
SLOTS = 4
LANES = 128
FORWARDS = (0.45, 0.75)
KINDS = {
    "c": (PLACE[0] * OWN, OWN, PLACE[1] * OWN, C),
    "x": (PLACE[0] * OWN, OWN, PLACE[4] * OWN, X),
    "y": (PLACE[0] * OWN, OWN, PLACE[2] * OWN, Y),
    "xc": (PLACE[4] * OWN, OWN, PLACE[5] * OWN, C),
    "yc": (PLACE[2] * OWN, OWN, PLACE[3] * OWN, C),
    "dt": (PLACE[4] * OWN, OWN // 2, PLACE[6] * OWN, Y),
    "db": (PLACE[2] * OWN + OWN // 2, OWN // 2, PLACE[6] * OWN + OWN // 2, X),
    "dc": (PLACE[6] * OWN, OWN, PLACE[7] * OWN, C),
}


def _gather_matmul(*refs, n, epilogue, early):
    x_ref, gain_ref = refs[:2]
    w_refs = refs[2 : 2 + n]
    outs = refs[2 + n : -6]
    all_s, acc_s, ring, w_sem, s_sem, r_sem = refs[-6:]
    chunks, steps = all_s.shape[0], acc_s.shape[0]
    d = chunks * KC
    rows = N * OWN
    cut = early == chunks
    uses = (early + chunks + cut) * steps

    def load(u):
        c = lax.div(u, steps)
        c = jnp.minimum(c - jnp.where(c < early, 0, early), chunks - 1)
        s = lax.rem(u, steps)
        return [
            pltpu.make_async_copy(
                w.at[pl.ds(pl.multiple_of(c * KC, KC), KC), pl.ds(pl.multiple_of(s * WIDE, WIDE), WIDE)],
                ring.at[lax.rem(u, SLOTS), :, pl.ds(i * WIDE, WIDE)],
                w_sem.at[lax.rem(u, SLOTS), i],
            )
            for i, w in enumerate(w_refs)
        ]

    def copy(kind, c):
        at, size, to, bit = KINDS[kind]
        i = list(KINDS).index(kind)
        return pltpu.make_async_remote_copy(
            src_ref=all_s.at[c, pl.ds(at, size)], dst_ref=all_s.at[c, pl.ds(to, size)], send_sem=s_sem.at[i, c], recv_sem=r_sem.at[i, c],
            device_id=_peer(bit), device_id_type=MESH)

    def start(c, *kinds):
        for kind in kinds:
            copy(kind, c).start()

    def wait(c, *kinds):
        for kind in kinds:
            copy(kind, c).wait_recv()

    def when(flag, then):
        if isinstance(flag, bool):
            if flag:
                then()
        else:
            pl.when(flag)(then)

    def forward(c):
        wait(c, "x", "y")
        start(c, "dt", "db", "xc", "yc")
        when(c + 2 < chunks, lambda: start(c + 2, "x", "y"))

    def finish(c):
        wait(c, "dt", "db")
        start(c, "dc")

    for u in range(SLOTS - 1):
        for part in load(u):
            part.start()

    def norm(i, _):
        some = pl.ds(pl.multiple_of(i * 16, 16), 16)
        squares = jnp.zeros((16, LANES), jnp.float32)
        for j in range(d // LANES):
            wide = x_ref[some, j * LANES : (j + 1) * LANES].astype(jnp.float32)
            squares += wide * wide
        scale = lax.rsqrt(jnp.sum(squares, axis=1, keepdims=True) * (1 / d) + 1e-6)
        for j in range(d // LANES):
            wide = x_ref[some, j * LANES : (j + 1) * LANES].astype(jnp.float32)
            at = j * LANES % KC
            all_s[j * LANES // KC, some, at : at + LANES] = (wide * scale * gain_ref[j : j + 1, :].astype(jnp.float32)).astype(jnp.bfloat16)

    lax.fori_loop(0, OWN // 16, norm, None)
    _meet()
    start(0, "x", "y")
    start(1, "x", "y")
    lax.fori_loop(0, chunks, lambda c, _: start(c, "c"), None)

    def block(u, c, at, size, mode):
        s, slot = lax.rem(u, steps), lax.rem(u, SLOTS)

        @pl.when(u + SLOTS - 1 < uses)
        def _():
            for part in load(u + SLOTS - 1):
                part.start()

        for part in load(u):
            part.wait()
        got = _dot(all_s[c, at : at + size, :], ring[slot], 1, 0)
        if mode != "first":
            got += acc_s[s, at : at + size, :]
        if mode != "last":
            acc_s[s, at : at + size, :] = got
        else:
            epilogue([got[:, i * WIDE : (i + 1) * WIDE] for i in range(n)], outs, slice(at, at + size), pl.ds(pl.multiple_of(s * WIDE, WIDE), WIDE))

    def run(first, c, at, size, mode, before=None):
        def body(s, _):
            if before is not None:
                before(s)
            block(first + s, c, at, size, mode)

        lax.fori_loop(0, steps, body, None)

    def first_rows(c, mode):
        wait(c, "c")

        def before(s):
            for k, share in enumerate(FORWARDS):
                pl.when(c * steps + s == int(early * steps * share))(lambda k=k: forward(k))

        run(c * steps, c, 0, 2 * OWN, mode, before)

    first_rows(0, "first")
    lax.fori_loop(1, chunks - 1 if cut else early, lambda c, _: first_rows(c, "middle"), None)
    if cut:
        first_rows(chunks - 1, "last")
    finish(0)

    def chunk(c, at, mode):
        wait(c, *(("xc", "yc", "dc") if at else ("c", "xc", "yc", "dc")))

        def before(s):
            pl.when((s == 0) & (c + 2 < chunks))(lambda: forward(c + 2))
            pl.when((s == steps - 1) & (c + 1 < chunks - cut))(lambda: finish(c + 1))

        run((early + c) * steps, c, at, rows - at, mode, before)

    chunk(0, 2 * OWN, "first")
    lax.fori_loop(1, chunks - 1 if cut else early, lambda c, _: chunk(c, 2 * OWN, "middle"), None)
    c = chunks - 1
    if cut:
        wait(c, "xc", "yc")
        run((early + c) * steps, c, 2 * OWN, 4 * OWN, "last")
        finish(c)
        wait(c, "dc")
        run((early + c + 1) * steps, c, 6 * OWN, 2 * OWN, "last")
    else:
        lax.fori_loop(early, c, lambda c, _: chunk(c, 0, "middle"), None)
        chunk(c, 0, "last")

    def drain(c, _):
        for kind in KINDS:
            copy(kind, c).wait_send()

    lax.fori_loop(0, chunks, drain, None)


def gather_matmul(x, gain, weights, outs, epilogue, collective_id, early, name):
    own, d = x.shape
    rows, width, n = N * own, weights[0].shape[1], len(weights)
    chunks, steps = d // KC, width // WIDE
    return pl.pallas_call(
        functools.partial(_gather_matmul, n=n, epilogue=epilogue, early=early),
        in_specs=[INSIDE, INSIDE] + [ANY] * n,
        out_specs=[INSIDE] * outs,
        out_shape=[jax.ShapeDtypeStruct((rows, width), jnp.bfloat16)] * outs,
        scratch_shapes=[
            pltpu.VMEM((chunks, rows, KC), jnp.bfloat16),
            pltpu.VMEM((steps, rows, n * WIDE), jnp.float32),
            pltpu.VMEM((SLOTS, KC, n * WIDE), jnp.bfloat16),
            pltpu.SemaphoreType.DMA((SLOTS, n)),
            pltpu.SemaphoreType.DMA((len(KINDS), chunks)),
            pltpu.SemaphoreType.DMA((len(KINDS), chunks)),
        ],
        compiler_params=pltpu.CompilerParams(collective_id=collective_id, has_side_effects=True, vmem_limit_bytes=BIG),
        cost_estimate=pl.CostEstimate(flops=2 * rows * d * width * n, transcendentals=0, bytes_accessed=2 * d * width * n),
        name=name,
    )(x, gain.reshape(-1, LANES), *weights)


def rounded(parts, outs, rows, columns):
    for part, out in zip(parts, outs):
        out[rows, columns] = part.astype(jnp.bfloat16)


def gated(parts, outs, rows, columns):
    gate, up = parts
    outs[0][rows, columns] = (gate * (1 / (1 + jnp.exp(-gate))) * up).astype(jnp.bfloat16)


NC = 256
LAGS = (10, 6, 2)
MULTIPLY_FIRST = False
KEEP = 12
HALF = OWN // 2


def _matmul_scatter(t_ref, res_ref, w_ref, out_ref, ring, away, mine, d_s, x_s, y_s, c_r, low_r, high_r, x_r, y_r, w_sem, s_sem, r_sem):
    chunks = c_r.shape[0]
    top, bottom = pl.ds(0, HALF), pl.ds(HALF, HALF)

    def load(i):
        return pltpu.make_async_copy(w_ref.at[:, pl.ds(pl.multiple_of(i * NC, NC), NC)], ring.at[lax.rem(i, SLOTS)], w_sem.at[lax.rem(i, SLOTS)])

    def copy(kind, i):
        k = lax.rem(i, KEEP)
        src, dst, bit = {
            "c": (away.at[k], c_r.at[i], C),
            "low": (d_s.at[k, top], low_r.at[i], X),
            "high": (d_s.at[k, bottom], high_r.at[i], Y),
            "x0": (x_s.at[k, top], x_r.at[i, top], X),
            "x1": (x_s.at[k, bottom], x_r.at[i, bottom], X),
            "y0": (y_s.at[k, top], y_r.at[i, top], Y),
            "y1": (y_s.at[k, bottom], y_r.at[i, bottom], Y),
        }[kind]
        j = ("c", "low", "high", "x0", "x1", "y0", "y1").index(kind)
        return pltpu.make_async_remote_copy(src_ref=src, dst_ref=dst, send_sem=s_sem.at[j, i], recv_sem=r_sem.at[j, i], device_id=_peer(bit),
                                            device_id_type=MESH)

    for i in range(SLOTS - 1):
        load(i).start()
    _meet()

    def multiply(i):
        k = lax.rem(i, KEEP)

        @pl.when(i + SLOTS - 1 < chunks)
        def _():
            load(i + SLOTS - 1).start()

        load(i).wait()
        got = _dot(t_ref[...], ring[lax.rem(i, SLOTS)], 1, 0)
        for b in range(4):
            away[k, b * OWN : (b + 1) * OWN, :] = got[(2 * b + 1) * OWN : (2 * b + 2) * OWN, :].astype(jnp.bfloat16)
            mine[k, b * OWN : (b + 1) * OWN, :] = got[2 * b * OWN : (2 * b + 1) * OWN, :]
        copy("c", i).start()

    def pair(i):
        k = lax.rem(i, KEEP)
        copy("c", i).wait_recv()
        sums = [mine[k, b * OWN : (b + 1) * OWN, :] + c_r[i, b * OWN : (b + 1) * OWN, :].astype(jnp.float32) for b in range(4)]
        d_s[k] = sums[3].astype(jnp.bfloat16)
        x_s[k, :HALF, :] = sums[1][:HALF].astype(jnp.bfloat16)
        y_s[k, HALF:, :] = sums[2][HALF:].astype(jnp.bfloat16)
        for kind in ("low", "high", "x0", "y1"):
            copy(kind, i).start()
        for b in range(3):
            mine[k, b * OWN : (b + 1) * OWN, :] = sums[b]
        copy("c", i).wait_send()

    def pass_on(i):
        k = lax.rem(i, KEEP)
        copy("low", i).wait_recv()
        y_s[k, :HALF, :] = (mine[k, 2 * OWN : 2 * OWN + HALF, :] + low_r[i].astype(jnp.float32)).astype(jnp.bfloat16)
        copy("y0", i).start()
        copy("high", i).wait_recv()
        x_s[k, HALF:, :] = (mine[k, OWN + HALF : 2 * OWN, :] + high_r[i].astype(jnp.float32)).astype(jnp.bfloat16)
        copy("x1", i).start()

    def finish(i):
        k = lax.rem(i, KEEP)
        for kind in ("x0", "x1", "y0", "y1"):
            copy(kind, i).wait_recv()
        columns = pl.ds(pl.multiple_of(i * NC, NC), NC)
        total = mine[k, :OWN, :] + x_r[i].astype(jnp.float32) + y_r[i].astype(jnp.float32)
        out_ref[:, columns] = (res_ref[:, columns].astype(jnp.float32) + total).astype(jnp.bfloat16)
        for kind in ("low", "high", "x0", "x1", "y0", "y1"):
            copy(kind, i).wait_send()

    def step(i, _):
        if MULTIPLY_FIRST:
            pl.when(i < chunks)(lambda: multiply(i))
        for lag, stage in zip(LAGS, (finish, pass_on, pair)):
            pl.when((i >= lag) & (i < chunks + lag))(lambda lag=lag, stage=stage: stage(i - lag))
        if not MULTIPLY_FIRST:
            pl.when(i < chunks)(lambda: multiply(i))

    lax.fori_loop(0, chunks + LAGS[0], step, None)


def matmul_scatter(res, t, w, collective_id, name):
    rows, depth = t.shape
    d = w.shape[1]
    chunks = d // NC
    sent = lambda *shape: pltpu.VMEM((*shape, NC), jnp.bfloat16)
    return pl.pallas_call(
        _matmul_scatter,
        in_specs=[INSIDE, INSIDE, ANY],
        out_specs=INSIDE,
        out_shape=jax.ShapeDtypeStruct(res.shape, res.dtype),
        scratch_shapes=[
            pltpu.VMEM((SLOTS, depth, NC), jnp.bfloat16),
            sent(KEEP, rows // 2),
            pltpu.VMEM((KEEP, rows // 2, NC), jnp.float32),
            sent(KEEP, OWN), sent(KEEP, OWN), sent(KEEP, OWN),
            sent(chunks, rows // 2), sent(chunks, HALF), sent(chunks, HALF), sent(chunks, OWN), sent(chunks, OWN),
            pltpu.SemaphoreType.DMA((SLOTS,)),
            pltpu.SemaphoreType.DMA((7, chunks)),
            pltpu.SemaphoreType.DMA((7, chunks)),
        ],
        compiler_params=pltpu.CompilerParams(collective_id=collective_id, has_side_effects=True, vmem_limit_bytes=BIG),
        cost_estimate=pl.CostEstimate(flops=2 * rows * depth * d, transcendentals=0, bytes_accessed=2 * depth * d),
        name=name,
    )(t, res, w)


def solution(mesh):
    def step(x, gain_a, wq, wk, wv, wo, gain_m, w_gate, w_up, w_down):
        cos, sin = tables(N * x.shape[0])
        q, k, v = gather_matmul(x, gain_a, (wq, wk, wv), 3, rounded, 0, 8, "qkv")
        seen = attend(q, k, v, cos, sin)
        h = matmul_scatter(x, seen, wo, 1, "wo")
        (hidden,) = gather_matmul(h, gain_m, (w_gate, w_up), 1, gated, 2, 4, "gate_up")
        return matmul_scatter(h, hidden, w_down, 3, "down")

    tokens, columns, rows_of = P(("dp", "tp"), None), P(None, "tp"), P("tp", None)
    return jax.shard_map(
        step,
        mesh=mesh,
        in_specs=(tokens, P(None), columns, columns, columns, rows_of, P(None), columns, columns, rows_of),
        out_specs=tokens,
        check_vma=False,
    )
```
